32 devices in a mesh: tp: 4 (over x, core), cp: 8 (over z, y).
Axes of the slice: x: 2, y: 2, z: 4, core: 2. Of those that a mesh axis runs over, the one named last changes fastest.
Arguments:
- tokens: bfloat16 [128, 8192], P(('cp', 'tp')), may hold values from -6 to 6
- attention_gain: float32 [8192], replicated, may hold values from 0.1 to 1.9
- query_weight: bfloat16 [8192, 8192], P('cp', 'tp'), may hold values from -0.0625 to 0.0625
- key_weight: bfloat16 [8192, 1024], P('cp', 'tp'), may hold values from -0.0625 to 0.0625
- value_weight: bfloat16 [8192, 1024], P('cp', 'tp'), may hold values from -0.0625 to 0.0625
- out_weight: bfloat16 [8192, 8192], P('tp', 'cp'), may hold values from -0.0625 to 0.0625
- feed_gain: float32 [8192], replicated, may hold values from 0.1 to 1.9
- gate_weight: bfloat16 [8192, 28672], P('tp', 'cp'), may hold values from -0.0625 to 0.0625
- up_weight: bfloat16 [8192, 28672], P('tp', 'cp'), may hold values from -0.0625 to 0.0625
- down_weight: bfloat16 [28672, 8192], P('cp', 'tp'), may hold values from -0.03125 to 0.03125
Outputs:
- attended: bfloat16 [128, 8192], P(('cp', 'tp'))
- mixed: bfloat16 [128, 8192], P(('cp', 'tp'))
The draws below stay inside these ranges and needn't reach their ends.
All inputs are finite; a program needn't handle non-finite values.
Results may differ from the reference program's by a relative error of at most 0.035.
Values may be sent and summed in bfloat16 or wider, within the bound.
A program may use at most 128 MiB of HBM per device.

```python
import jax
import jax.numpy as jnp
from jax import lax

D = 8192
HQ = 64
KV = 8
HD = 128
FF = 28672
SEQ = 128


def levels(own_key, shape, split, smallest, high):
    factor_of, own = 1.0, jax.random.fold_in(own_key, 6)
    for position, shards_of in split:
        steps = jnp.exp(jax.random.uniform(jax.random.fold_in(own, position), (shards_of,), jnp.float32, smallest / len(split), high / len(split)))
        factor_of = factor_of * jnp.repeat(steps, shape[position] // shards_of).reshape([-1 if axis == position else 1 for axis in range(len(shape))])
    return factor_of


def centred(key, extent, spread, bound, cuts=(), kind=jnp.bfloat16):
    result = spread * jax.random.normal(key, extent, jnp.float32)
    if cuts:
        result = result * levels(key, extent, cuts, -0.22, 0.18)
    return jnp.clip(result, -bound, bound).astype(kind)


def setup_inputs(seed: int = 0) -> dict:
    key_list = jax.random.split(jax.random.key(seed), 11)
    return {
        "tokens": centred(key_list[0], (SEQ, D), 0.5, 6.0, ((0, 32),)),
        "attention_gain": jnp.clip(1.0 + 0.18 * jax.random.normal(key_list[1], (D,), jnp.float32), 0.1, 1.9),
        "query_weight": centred(key_list[2], (D, HQ * HD), D ** -0.5, 0.0625, ((0, 8), (1, 4))),
        "key_weight": centred(key_list[3], (D, KV * HD), D ** -0.5, 0.0625, ((0, 8), (1, 4))),
        "value_weight": centred(key_list[4], (D, KV * HD), D ** -0.5, 0.0625, ((0, 8), (1, 4))),
        "out_weight": centred(key_list[5], (HQ * HD, D), (HQ * HD) ** -0.5, 0.0625, ((0, 4), (1, 8))),
        "feed_gain": jnp.clip(1.0 + 0.18 * jax.random.normal(key_list[6], (D,), jnp.float32), 0.1, 1.9),
        "gate_weight": centred(key_list[7], (D, FF), D ** -0.5, 0.0625, ((0, 4), (1, 8))),
        "up_weight": centred(key_list[8], (D, FF), D ** -0.5, 0.0625, ((0, 4), (1, 8))),
        "down_weight": centred(key_list[9], (FF, D), FF ** -0.5, 0.03125, ((0, 8), (1, 4))),
    }


epsilon = 1e-05
rope_base = 500000.0

def normalize(values, gain):
    widened = values.astype(jnp.float32)
    mean_square = lax.optimization_barrier(jnp.mean(widened * widened, axis=-1, keepdims=True))
    return (widened * lax.rsqrt(mean_square + epsilon) * gain).astype(jnp.bfloat16)

def rotate(values, positions):
    row_count = values.shape[0]
    heads = values.reshape(row_count, -1, HD)
    half = HD // 2
    inverse = rope_base ** (-(jnp.arange(half, dtype=jnp.float32) * 2.0 / HD))
    angles = positions.astype(jnp.float32)[:, None] * inverse[None, :]
    cosine = jnp.cos(angles)[:, None, :]
    sine = jnp.sin(angles)[:, None, :]
    first = heads[..., :half]
    second = heads[..., half:]
    turned = jnp.concatenate([first * cosine - second * sine, second * cosine + first * sine], axis=-1)
    return turned.reshape(row_count, -1)

def reference(tokens, attention_gain, query_weight, key_weight, value_weight, out_weight, feed_gain, gate_weight, up_weight, down_weight):
    normed = normalize(tokens, attention_gain)
    positions = jnp.arange(SEQ, dtype=jnp.int32)
    query = rotate(jnp.dot(normed, query_weight, preferred_element_type=jnp.float32), positions).astype(jnp.bfloat16)
    keys = rotate(jnp.dot(normed, key_weight, preferred_element_type=jnp.float32), positions).astype(jnp.bfloat16)
    values = jnp.dot(normed, value_weight, preferred_element_type=jnp.float32).astype(jnp.bfloat16)
    group_size = HQ // KV
    query_heads = query.astype(jnp.float32).reshape(SEQ, KV, group_size, HD).transpose(1, 0, 2, 3)
    key_heads = keys.astype(jnp.float32).reshape(SEQ, KV, HD).transpose(1, 0, 2)
    value_heads = values.astype(jnp.float32).reshape(SEQ, KV, HD).transpose(1, 0, 2)
    allowed = positions[None, :] <= positions[:, None]
    scale = HD ** (-0.5)

    def one_head(operands):
        head_query, head_keys, head_values = operands
        scores = jnp.einsum('qgd,sd->gqs', head_query, head_keys, precision=lax.Precision.HIGHEST) * scale
        scores = jnp.where(allowed[None], scores, -1e+30)
        weights = jax.nn.softmax(scores, axis=-1)
        return jnp.einsum('gqs,sd->qgd', weights, head_values, precision=lax.Precision.HIGHEST)
    head_outputs = lax.map(one_head, (query_heads, key_heads, value_heads))
    attention = head_outputs.transpose(1, 0, 2, 3).reshape(SEQ, HQ * HD).astype(jnp.bfloat16)
    projected = jnp.dot(attention, out_weight, preferred_element_type=jnp.float32)
    attended = (tokens.astype(jnp.float32) + projected).astype(jnp.bfloat16)
    normed_feed = normalize(attended, feed_gain)
    gate = jnp.dot(normed_feed, gate_weight, preferred_element_type=jnp.float32)
    upward = jnp.dot(normed_feed, up_weight, preferred_element_type=jnp.float32)
    hidden = (jax.nn.silu(gate) * upward).astype(jnp.bfloat16)
    lowered = jnp.dot(hidden, down_weight, preferred_element_type=jnp.float32)
    mixed = (attended.astype(jnp.float32) + lowered).astype(jnp.bfloat16)
    return (attended, mixed)
```

```python
import functools

import jax
import jax.numpy as jnp
import numpy as np
from jax import lax
from jax.experimental import pallas as pl
from jax.experimental.pallas import tpu as pltpu
from jax.sharding import PartitionSpec as P

HD = 128
epsilon = 1e-05
rope_base = 500000.0
masked = -1e30
bf16 = jnp.bfloat16
f32 = jnp.float32
MESH = pl.DeviceIdType.MESH


def tile_of(width, most=512):
    for size in (512, 256, 128):
        if size <= most and width % size == 0:
            return size
    return width


def normalize(values, gain):
    mean_square = jnp.mean(values * values, axis=-1, keepdims=True)
    return (values * lax.rsqrt(mean_square + epsilon) * gain).astype(bf16)


def kernel(
    T,
    C,
    tokens,
    again,
    fgain,
    cosine,
    sine,
    wq_h,
    wk_h,
    wv_h,
    wo_h,
    wg_h,
    wu_h,
    wd_h,
    attended_ref,
    mixed_ref,
    wq,
    wk,
    wv,
    wo,
    wg,
    wu,
    wd,
    xsend,
    xrecv,
    xb,
    stage,
    psend,
    precv,
    kvbuf,
    abuf,
    osend,
    orecv,
    nsend,
    nrecv,
    gu,
    g1recv,
    g2send,
    g2recv,
    hid,
    dsend,
    drecv,
    wsem,
    lsem,
    ssem,
    rsem,
):
    G = C * T
    X = T // 2
    R = tokens.shape[0]
    B = R * T
    N = R * G
    c_me = lax.axis_index("cp")
    t_me = lax.axis_index("tp")
    g_me = c_me * T + t_me
    x_me = lax.div(t_me, 2)
    core = lax.rem(t_me, 2)
    QW = wq.shape[1]
    KW = wk.shape[1]
    DC = wq.shape[0]
    DT = wg.shape[0]
    FW = wg.shape[1]

    weights = [(wq_h, wq), (wk_h, wk), (wv_h, wv), (wo_h, wo), (wg_h, wg), (wu_h, wu), (wd_h, wd)]
    loads = [pltpu.make_async_copy(s, d, wsem.at[i]) for i, (s, d) in enumerate(weights)]

    barrier = pltpu.get_barrier_semaphore()

    @pl.loop(1, G)
    def _(k):
        g = lax.rem(g_me + k, G)
        pl.semaphore_signal(
            barrier, inc=1, device_id={"cp": lax.div(g, T), "tp": lax.rem(g, T)}, device_id_type=MESH
        )

    for load in loads:
        load.start()

    normed = normalize(tokens[...].astype(f32), again[...])
    for c in range(C):
        xsend[c] = normed[:, c * DC : (c + 1) * DC]
    pl.semaphore_wait(barrier, G - 1)

    def remote(src, dst, phase, cp, tp):
        return pltpu.make_async_remote_copy(
            src_ref=src,
            dst_ref=dst,
            send_sem=ssem.at[phase],
            recv_sem=rsem.at[phase],
            device_id={"cp": cp, "tp": tp},
            device_id_type=MESH,
        )

    def to_all(source, buffer, phase):
        own = pltpu.make_async_copy(source(c_me, t_me, g_me), buffer.at[g_me], lsem.at[phase])
        own.start()

        @pl.loop(1, G)
        def _(k):
            g = lax.rem(g_me + k, G)
            c = lax.div(g, T)
            t = lax.rem(g, T)
            remote(source(c, t, g), buffer.at[g_me], phase, c, t).start()

        return own

    def to_cp(source, buffer, phase):
        @pl.loop(1, C)
        def _(k):
            c = lax.rem(c_me + k, C)
            remote(source(c), buffer.at[c_me], phase, c, t_me).start()

    def bytes_wait(view, sem):
        pltpu.make_async_copy(view, view, sem).wait()

    own = to_all(lambda c, t, g: xsend.at[c], xrecv, 0)
    own.wait()
    bytes_wait(xrecv.at[pl.ds(0, G - 1)], rsem.at[0])
    for g in range(G):
        stage[g * R : (g + 1) * R, :DC] = xrecv[g].astype(f32)
    xb[:, :DC] = stage[:, :DC].astype(bf16)

    def project(weight, width, base):
        size = tile_of(width)

        @pl.loop(0, width // size)
        def _(n):
            at = pl.multiple_of(n * size, size)
            part = jnp.dot(xb[:, :DC], weight[:, pl.ds(at, size)], preferred_element_type=f32)
            psend[:, :, pl.ds(pl.multiple_of(base + at, 128), size)] = part.reshape(C, B, size).astype(bf16)

    loads[0].wait()
    project(wq, QW, 0)
    loads[1].wait()
    project(wk, KW, QW)
    loads[2].wait()
    project(wv, KW, QW + KW)
    to_cp(lambda c: psend.at[c], precv, 1)
    bytes_wait(precv.at[pl.ds(0, C - 1)], rsem.at[1])

    row0 = pl.multiple_of(c_me * B, B)
    cos = cosine[pl.ds(row0, B), :]
    sin = sine[pl.ds(row0, B), :]

    def summed(at, width):
        total = psend[c_me, :, at : at + width].astype(f32)
        for k in range(1, C):
            total += precv[lax.rem(c_me + k, C), :, at : at + width].astype(f32)
        return total

    def turned(head):
        return (head * cos + pltpu.roll(head, HD // 2, 1) * sin).astype(bf16)

    heads = QW // HD
    shared = KW // HD
    group = heads // shared
    for h in range(shared):
        kvbuf[c_me, :, h * HD : (h + 1) * HD] = turned(summed(QW + h * HD, HD))
    kvbuf[c_me, :, KW:] = summed(QW + KW, KW).astype(bf16)
    to_cp(lambda c: kvbuf.at[c_me], kvbuf, 2)
    queries = [turned(summed(h * HD, HD)) for h in range(heads)]
    bytes_wait(kvbuf.at[pl.ds(0, C - 1)], rsem.at[2])

    scale = HD ** (-0.5)
    for s in range(shared):
        q = jnp.concatenate(queries[s * group : (s + 1) * group], axis=0)
        keys = kvbuf[:, :, s * HD : (s + 1) * HD].reshape(N, HD)
        vals = kvbuf[:, :, KW + s * HD : KW + (s + 1) * HD].reshape(N, HD)
        scores = (
            lax.dot_general(q, keys, (((1,), (1,)), ((), ())), preferred_element_type=f32) * scale
        )
        rows = lax.broadcasted_iota(jnp.int32, (group * B, N), 0)
        cols = lax.broadcasted_iota(jnp.int32, (group * B, N), 1)
        allowed = cols <= (rows & (B - 1)) + row0
        scores = jnp.where(allowed, scores, masked)
        top = jnp.max(scores, axis=-1, keepdims=True)
        soft = jnp.where(allowed, jnp.exp(scores - top), 0.0)
        total = jnp.sum(soft, axis=-1, keepdims=True)
        mix = jnp.dot(soft.astype(bf16), vals, preferred_element_type=f32) / total
        for j in range(group):
            h = s * group + j
            abuf[c_me, :, h * HD : (h + 1) * HD] = mix[j * B : (j + 1) * B].astype(bf16)
    to_cp(lambda c: abuf.at[c_me], abuf, 3)
    loads[3].wait()
    bytes_wait(abuf.at[pl.ds(0, C - 1)], rsem.at[3])

    OC = wo.shape[1]
    osize = tile_of(OC)

    @pl.loop(0, OC // osize)
    def _(n):
        at = pl.multiple_of(n * osize, osize)
        stage[:, pl.ds(at, osize)] = jnp.dot(
            abuf[...].reshape(N, QW), wo[:, pl.ds(at, osize)], preferred_element_type=f32
        )

    for g in range(G):
        osend[g] = stage[g * R : (g + 1) * R, :OC].astype(bf16)
    own = to_all(lambda c, t, g: osend.at[g], orecv, 4)
    own.wait()
    bytes_wait(orecv.at[pl.ds(0, G - 1)], rsem.at[4])
    for c in range(C):
        total = tokens[:, c * OC : (c + 1) * OC].astype(f32)
        add = orecv[c * T].astype(f32)
        for t in range(1, T):
            add += orecv[c * T + t].astype(f32)
        attended_ref[:, c * OC : (c + 1) * OC] = (total + add).astype(bf16)

    normed_feed = normalize(attended_ref[...].astype(f32), fgain[...])
    for t in range(T):
        nsend[t] = normed_feed[:, t * DT : (t + 1) * DT]
    own = to_all(lambda c, t, g: nsend.at[t], nrecv, 5)
    loads[4].wait()
    loads[5].wait()
    own.wait()
    bytes_wait(nrecv.at[pl.ds(0, G - 1)], rsem.at[5])
    for g in range(G):
        stage[g * R : (g + 1) * R, :DT] = nrecv[g].astype(f32)
    xb[:, :DT] = stage[:, :DT].astype(bf16)

    fsize = tile_of(FW)
    share = N // T

    @pl.loop(0, FW // fsize)
    def _(n):
        at = pl.multiple_of(n * fsize, fsize)
        for weight, base in ((wg, 0), (wu, FW)):
            part = jnp.dot(xb[:, :DT], weight[:, pl.ds(at, fsize)], preferred_element_type=f32)
            gu[:, :, pl.ds(pl.multiple_of(base + at, 128), fsize)] = part.reshape(T, share, fsize).astype(bf16)

    @pl.loop(0, X)
    def _(x):
        remote(gu.at[2 * x + 1 - core], g1recv.at[x], 6, c_me, 2 * x_me + 1 - core).start()

    bytes_wait(g1recv, rsem.at[6])
    tiles = 2 * FW // fsize
    for k in range(1, X):
        x = lax.rem(x_me + k, X)

        @pl.loop(0, tiles)
        def _(n):
            cols = pl.ds(pl.multiple_of(n * fsize, fsize), fsize)
            g2send[k - 1, :, cols] = (
                gu[2 * x + core, :, cols].astype(f32) + g1recv[x, :, cols].astype(f32)
            ).astype(bf16)

        remote(g2send.at[k - 1], g2recv.at[k - 1], 7, c_me, 2 * x + core).start()
    if X > 1:
        bytes_wait(g2recv, rsem.at[7])

    def unit(cols):
        total = gu[t_me, :, cols].astype(f32) + g1recv[x_me, :, cols].astype(f32)
        for k in range(1, X):
            total += g2recv[k - 1, :, cols].astype(f32)
        return total

    @pl.loop(0, FW // fsize)
    def _(n):
        at = pl.multiple_of(n * fsize, fsize)
        gate = unit(pl.ds(at, fsize))
        up = unit(pl.ds(pl.multiple_of(FW + at, 128), fsize))
        hid[t_me, :, pl.ds(at, fsize)] = (gate / (1.0 + jnp.exp(-gate)) * up).astype(bf16)

    partner = 2 * x_me + 1 - core
    for k in range(1, X):
        remote(hid.at[t_me], hid.at[t_me], 8, c_me, 2 * lax.rem(x_me + k, X) + core).start()
    remote(hid.at[t_me], hid.at[t_me], 9, c_me, partner).start()
    if X > 1:
        bytes_wait(hid.at[pl.ds(0, X - 1)], rsem.at[8])
        for k in range(1, X):
            t = 2 * lax.rem(x_me + k, X) + core
            remote(hid.at[t], hid.at[t], 9, c_me, partner).start()
    loads[6].wait()
    bytes_wait(hid.at[pl.ds(0, X)], rsem.at[9])

    DW = wd.shape[1]
    dsize = tile_of(DW, 256)

    @pl.loop(0, DW // dsize)
    def _(n):
        at = pl.multiple_of(n * dsize, dsize)
        stage[:, pl.ds(at, dsize)] = jnp.dot(
            hid[...].reshape(N, FW), wd[:, pl.ds(at, dsize)], preferred_element_type=f32
        )

    for g in range(G):
        dsend[g] = stage[g * R : (g + 1) * R, :DW].astype(bf16)
    own = to_all(lambda c, t, g: dsend.at[g], drecv, 10)
    own.wait()
    bytes_wait(drecv.at[pl.ds(0, G - 1)], rsem.at[10])
    for t in range(T):
        add = drecv[t].astype(f32)
        for c in range(1, C):
            add += drecv[c * T + t].astype(f32)
        cols = slice(t * DW, (t + 1) * DW)
        mixed_ref[:, cols] = (attended_ref[:, cols].astype(f32) + add).astype(bf16)

    bytes_wait(xrecv.at[pl.ds(0, G - 1)], ssem.at[0])
    bytes_wait(precv.at[pl.ds(0, C - 1)], ssem.at[1])
    bytes_wait(kvbuf.at[pl.ds(0, C - 1)], ssem.at[2])
    bytes_wait(abuf.at[pl.ds(0, C - 1)], ssem.at[3])
    bytes_wait(orecv.at[pl.ds(0, G - 1)], ssem.at[4])
    bytes_wait(nrecv.at[pl.ds(0, G - 1)], ssem.at[5])
    bytes_wait(g1recv, ssem.at[6])
    if X > 1:
        bytes_wait(g2recv, ssem.at[7])
        bytes_wait(hid.at[pl.ds(0, X - 1)], ssem.at[8])
    bytes_wait(hid.at[pl.ds(0, X)], ssem.at[9])
    bytes_wait(drecv.at[pl.ds(0, G - 1)], ssem.at[10])


def tables(count):
    half = HD // 2
    inverse = rope_base ** (-(np.arange(half, dtype=np.float64) * 2.0 / HD))
    angles = np.arange(count, dtype=np.float64)[:, None] * inverse[None, :]
    cos = np.concatenate([np.cos(angles), np.cos(angles)], axis=1)
    sin = np.concatenate([-np.sin(angles), np.sin(angles)], axis=1)
    return jnp.asarray(cos, f32), jnp.asarray(sin, f32)


def per_device(tokens, again, wq, wk, wv, wo, fgain, wg, wu, wd, *, T, C):
    R, D = tokens.shape
    G = T * C
    X = T // 2
    N = R * G
    B = R * T
    QW, KW, FW = wq.shape[1], wk.shape[1], wg.shape[1]
    DC, DT, OC, DW = wq.shape[0], wg.shape[0], wo.shape[1], wd.shape[1]
    cos, sin = tables(N)
    vm = pl.BlockSpec(memory_space=pltpu.VMEM)
    hbm = pl.BlockSpec(memory_space=pl.ANY)
    wide = max(DC, DT, OC, DW)

    def buf(*shape, dtype=bf16):
        return pltpu.VMEM(shape, dtype)

    macs = N * sum(w.size for w in (wq, wk, wv, wo, wg, wu, wd))
    return pl.pallas_call(
        functools.partial(kernel, T, C),
        out_shape=(jax.ShapeDtypeStruct((R, D), bf16), jax.ShapeDtypeStruct((R, D), bf16)),
        in_specs=[vm] * 5 + [hbm] * 7,
        out_specs=(vm, vm),
        scratch_shapes=[
            *[buf(*w.shape) for w in (wq, wk, wv, wo, wg, wu, wd)],
            buf(C, R, DC),
            buf(G, R, DC),
            buf(N, max(DC, DT)),
            buf(N, wide, dtype=f32),
            buf(C, B, QW + 2 * KW),
            buf(C, B, QW + 2 * KW),
            buf(C, B, 2 * KW),
            buf(C, B, QW),
            buf(G, R, OC),
            buf(G, R, OC),
            buf(T, R, DT),
            buf(G, R, DT),
            buf(T, N // T, 2 * FW),
            buf(X, N // T, 2 * FW),
            buf(max(X - 1, 1), N // T, 2 * FW),
            buf(max(X - 1, 1), N // T, 2 * FW),
            buf(T, N // T, FW),
            buf(G, R, DW),
            buf(G, R, DW),
            pltpu.SemaphoreType.DMA((7,)),
            pltpu.SemaphoreType.DMA((11,)),
            pltpu.SemaphoreType.DMA((11,)),
            pltpu.SemaphoreType.DMA((11,)),
        ],
        compiler_params=pltpu.CompilerParams(
            collective_id=0, has_side_effects=True, vmem_limit_bytes=67043328
        ),
        cost_estimate=pl.CostEstimate(flops=2 * macs, bytes_accessed=2 * macs // N, transcendentals=0),
    )(tokens, again.reshape(1, D), fgain.reshape(1, D), cos, sin, wq, wk, wv, wo, wg, wu, wd)


def solution(mesh):
    in_specs = (
        P(("cp", "tp"), None),
        P(),
        P("cp", "tp"),
        P("cp", "tp"),
        P("cp", "tp"),
        P("tp", "cp"),
        P(),
        P("tp", "cp"),
        P("tp", "cp"),
        P("cp", "tp"),
    )
    out_specs = (P(("cp", "tp"), None), P(("cp", "tp"), None))
    body = functools.partial(per_device, T=mesh.shape["tp"], C=mesh.shape["cp"])
    return jax.shard_map(body, mesh=mesh, in_specs=in_specs, out_specs=out_specs, check_vma=False)
```

```python
import functools

import jax
import jax.numpy as jnp
import numpy as np
from jax import lax
from jax.experimental import pallas as pl
from jax.experimental.pallas import tpu as pltpu
from jax.sharding import PartitionSpec as P

HD = 128
epsilon = 1e-05
rope_base = 500000.0
masked = -1e30
bf16 = jnp.bfloat16
f32 = jnp.float32
MESH = pl.DeviceIdType.MESH


def tile_of(width, most=512):
    for size in (512, 256, 128):
        if size <= most and width % size == 0:
            return size
    return width


def normalize(values, gain):
    mean_square = jnp.mean(values * values, axis=-1, keepdims=True)
    return (values * lax.rsqrt(mean_square + epsilon) * gain).astype(bf16)


def kernel(
    T,
    C,
    tokens,
    again,
    fgain,
    cosine,
    sine,
    wq_h,
    wk_h,
    wv_h,
    wo_h,
    wg_h,
    wu_h,
    wd_h,
    attended_ref,
    mixed_ref,
    wq,
    wk,
    wv,
    wo,
    wg,
    wu,
    wd,
    xsend,
    xrecv,
    xb,
    stage,
    psend,
    precv,
    kvbuf,
    abuf,
    osend,
    orecv,
    nsend,
    nrecv,
    gu,
    g1recv,
    g2send,
    g2recv,
    hid,
    dsend,
    drecv,
    wsem,
    lsem,
    ssem,
    rsem,
    asem,
    bsem,
    r1sem,
    r2sem,
    r8sem,
):
    G = C * T
    X = T // 2
    R = tokens.shape[0]
    B = R * T
    N = R * G
    c_me = lax.axis_index("cp")
    t_me = lax.axis_index("tp")
    g_me = c_me * T + t_me
    x_me = lax.div(t_me, 2)
    core = lax.rem(t_me, 2)
    QW = wq.shape[1]
    KW = wk.shape[1]
    DC = wq.shape[0]
    DT = wg.shape[0]
    FW = wg.shape[1]

    weights = [(wq_h, wq), (wk_h, wk), (wv_h, wv), (wo_h, wo), (wg_h, wg), (wu_h, wu), (wd_h, wd)]
    loads = [pltpu.make_async_copy(s, d, wsem.at[i]) for i, (s, d) in enumerate(weights)]

    barrier = pltpu.get_barrier_semaphore()

    @pl.loop(1, G)
    def _(k):
        g = lax.rem(g_me + k, G)
        pl.semaphore_signal(
            barrier, inc=1, device_id={"cp": lax.div(g, T), "tp": lax.rem(g, T)}, device_id_type=MESH
        )

    for load in loads:
        load.start()

    normed = normalize(tokens[...].astype(f32), again[...])
    for c in range(C):
        xsend[c] = normed[:, c * DC : (c + 1) * DC]
    pl.semaphore_wait(barrier, G - 1)

    def remote(src, dst, phase, cp, tp, arrival=None):
        return pltpu.make_async_remote_copy(
            src_ref=src,
            dst_ref=dst,
            send_sem=ssem.at[phase],
            recv_sem=rsem.at[phase] if arrival is None else arrival,
            device_id={"cp": cp, "tp": tp},
            device_id_type=MESH,
        )

    def to_all(source, buffer, phase):
        own = pltpu.make_async_copy(source(c_me, t_me, g_me), buffer.at[g_me], lsem.at[phase])
        own.start()

        @pl.loop(1, G)
        def _(k):
            g = lax.rem(g_me + k, G)
            c = lax.div(g, T)
            t = lax.rem(g, T)
            remote(source(c, t, g), buffer.at[g_me], phase, c, t).start()

        return own

    def to_cp(source, buffer, phase):
        @pl.loop(1, C)
        def _(k):
            c = lax.rem(c_me + k, C)
            remote(source(c), buffer.at[c_me], phase, c, t_me).start()

    def bytes_wait(view, sem):
        pltpu.make_async_copy(view, view, sem).wait()

    def cp_gather(buffer, phase, sems):
        pair = c_me + 1 - 2 * lax.rem(c_me, 2)
        half = C // 2
        own = buffer.at[c_me]

        @pl.loop(1, half)
        def _(k):
            remote(own, own, phase, lax.rem(c_me + 2 * k, C), t_me, sems.at[k]).start()

        remote(own, own, phase, pair, t_me).start()

        @pl.loop(1, half)
        def _(k):
            came = buffer.at[lax.rem(c_me + C - 2 * k, C)]
            bytes_wait(came, sems.at[k])
            remote(came, came, phase, pair, t_me).start()

        bytes_wait(buffer.at[pl.ds(0, half)], rsem.at[phase])

    own = to_all(lambda c, t, g: xsend.at[c], xrecv, 0)
    own.wait()
    bytes_wait(xrecv.at[pl.ds(0, G - 1)], rsem.at[0])
    for g in range(G):
        stage[g * R : (g + 1) * R, :DC] = xrecv[g].astype(f32)
    xb[:, :DC] = stage[:, :DC].astype(bf16)

    def project(weight, width, base):
        size = tile_of(width)

        @pl.loop(0, width // size)
        def _(n):
            at = pl.multiple_of(n * size, size)
            part = jnp.dot(xb[:, :DC], weight[:, pl.ds(at, size)], preferred_element_type=f32)
            cols = pl.ds(pl.multiple_of(base + at, 128), size)
            psend[:, :, cols] = part.reshape(C, B, size).astype(bf16)

            @pl.loop(1, C)
            def _(k):
                c = lax.rem(c_me + k, C)
                remote(psend.at[c, :, cols], precv.at[c_me, :, cols], 1, c, t_me).start()

    loads[0].wait()
    project(wq, QW, 0)
    loads[1].wait()
    project(wk, KW, QW)
    loads[2].wait()
    project(wv, KW, QW + KW)
    bytes_wait(precv.at[pl.ds(0, C - 1)], rsem.at[1])

    row0 = pl.multiple_of(c_me * B, B)
    cos = cosine[pl.ds(row0, B), :]
    sin = sine[pl.ds(row0, B), :]

    def summed(at, width):
        total = psend[c_me, :, at : at + width].astype(f32)
        for k in range(1, C):
            total += precv[lax.rem(c_me + k, C), :, at : at + width].astype(f32)
        return total

    def turned(head):
        return (head * cos + pltpu.roll(head, HD // 2, 1) * sin).astype(bf16)

    heads = QW // HD
    shared = KW // HD
    group = heads // shared
    for h in range(shared):
        kvbuf[c_me, :, h * HD : (h + 1) * HD] = turned(summed(QW + h * HD, HD))
    kvbuf[c_me, :, KW:] = summed(QW + KW, KW).astype(bf16)
    to_cp(lambda c: kvbuf.at[c_me], kvbuf, 2)
    queries = [turned(summed(h * HD, HD)) for h in range(heads)]
    bytes_wait(kvbuf.at[pl.ds(0, C - 1)], rsem.at[2])

    scale = HD ** (-0.5)
    for s in range(shared):
        q = jnp.concatenate(queries[s * group : (s + 1) * group], axis=0)
        keys = kvbuf[:, :, s * HD : (s + 1) * HD].reshape(N, HD)
        vals = kvbuf[:, :, KW + s * HD : KW + (s + 1) * HD].reshape(N, HD)
        scores = (
            lax.dot_general(q, keys, (((1,), (1,)), ((), ())), preferred_element_type=f32) * scale
        )
        rows = lax.broadcasted_iota(jnp.int32, (group * B, N), 0)
        cols = lax.broadcasted_iota(jnp.int32, (group * B, N), 1)
        allowed = cols <= (rows & (B - 1)) + row0
        scores = jnp.where(allowed, scores, masked)
        top = jnp.max(scores, axis=-1, keepdims=True)
        soft = jnp.where(allowed, jnp.exp(scores - top), 0.0)
        total = jnp.sum(soft, axis=-1, keepdims=True)
        mix = jnp.dot(soft.astype(bf16), vals, preferred_element_type=f32) / total
        for j in range(group):
            h = s * group + j
            abuf[c_me, :, h * HD : (h + 1) * HD] = mix[j * B : (j + 1) * B].astype(bf16)
    cp_gather(abuf, 3, asem)
    loads[3].wait()

    OC = wo.shape[1]
    osize = tile_of(OC)

    @pl.loop(0, OC // osize)
    def _(n):
        at = pl.multiple_of(n * osize, osize)
        stage[:, pl.ds(at, osize)] = jnp.dot(
            abuf[...].reshape(N, QW), wo[:, pl.ds(at, osize)], preferred_element_type=f32
        )

    for g in range(G):
        osend[g] = stage[g * R : (g + 1) * R, :OC].astype(bf16)
    own = to_all(lambda c, t, g: osend.at[g], orecv, 4)
    own.wait()
    bytes_wait(orecv.at[pl.ds(0, G - 1)], rsem.at[4])
    for c in range(C):
        total = tokens[:, c * OC : (c + 1) * OC].astype(f32)
        add = orecv[c * T].astype(f32)
        for t in range(1, T):
            add += orecv[c * T + t].astype(f32)
        attended_ref[:, c * OC : (c + 1) * OC] = (total + add).astype(bf16)

    normed_feed = normalize(attended_ref[...].astype(f32), fgain[...])
    for t in range(T):
        nsend[t] = normed_feed[:, t * DT : (t + 1) * DT]
    own = pltpu.make_async_copy(nsend.at[t_me], nrecv.at[c_me, t_me], lsem.at[5])
    own.start()
    for k in range(1, T):
        t = lax.rem(t_me + k, T)
        remote(nsend.at[t], nrecv.at[c_me, t_me], 5, c_me, t).start()
    own.wait()
    bytes_wait(nrecv.at[0, pl.ds(0, T - 1)], rsem.at[5])
    cp_gather(nrecv, 11, bsem)
    loads[4].wait()
    loads[5].wait()
    for g in range(G):
        stage[g * R : (g + 1) * R, :DT] = nrecv[g // T, g % T].astype(f32)
    xb[:, :DT] = stage[:, :DT].astype(bf16)

    fsize = tile_of(FW)
    share = N // T

    tiles = FW // fsize
    partner = 2 * x_me + 1 - core

    def spans(n):
        at = n * fsize
        return [pl.ds(pl.multiple_of(base + at, 128), fsize) for base in (0, FW)]

    def compute(n):
        at = pl.multiple_of(n * fsize, 128)
        for weight, cols in zip((wg, wu), spans(n)):
            part = jnp.dot(xb[:, :DT], weight[:, pl.ds(at, fsize)], preferred_element_type=f32)
            gu[:, :, cols] = part.reshape(T, share, fsize).astype(bf16)
        for cols in spans(n):
            for x in range(X):
                remote(
                    gu.at[2 * x + 1 - core, :, cols],
                    g1recv.at[x, :, cols],
                    6,
                    c_me,
                    partner,
                    r1sem.at[n],
                ).start()

    def across(n):
        bytes_wait(g1recv.at[:, :, pl.ds(0, 2 * fsize)], r1sem.at[n])
        for k in range(1, X):
            x = lax.rem(x_me + k, X)
            for cols in spans(n):
                both = gu[2 * x + core, :, cols].astype(f32) + g1recv[x, :, cols].astype(f32)
                g2send[k - 1, :, cols] = both.astype(bf16)
            for cols in spans(n):
                remote(
                    g2send.at[k - 1, :, cols],
                    g2recv.at[k - 1, :, cols],
                    7,
                    c_me,
                    2 * x + core,
                    r2sem.at[n],
                ).start()

    @pl.loop(0, tiles)
    def _(n):
        compute(n)

        @pl.when(n >= 1)
        def _():
            across(n - 1)

    across(tiles - 1)

    def unit(cols):
        total = gu[t_me, :, cols].astype(f32) + g1recv[x_me, :, cols].astype(f32)
        for k in range(1, X):
            total += g2recv[k - 1, :, cols].astype(f32)
        return total

    def finish(n):
        if X > 1:
            bytes_wait(g2recv.at[:, :, pl.ds(0, 2 * fsize)], r2sem.at[n])
        cols, upper = spans(n)
        gate = unit(cols)
        up = unit(upper)
        hid[t_me, :, cols] = (gate / (1.0 + jnp.exp(-gate)) * up).astype(bf16)
        own = hid.at[t_me, :, cols]
        for k in range(1, X):
            x = lax.rem(x_me + k, X)
            remote(own, own, 8, c_me, 2 * x + core, r8sem.at[n]).start()
        remote(own, own, 9, c_me, partner).start()

    def forward(n):
        if X > 1:
            cols = spans(n)[0]
            bytes_wait(hid.at[pl.ds(0, X - 1), :, cols], r8sem.at[n])
            for k in range(1, X):
                came = hid.at[2 * lax.rem(x_me + k, X) + core, :, cols]
                remote(came, came, 9, c_me, partner).start()

    @pl.loop(0, tiles)
    def _(n):
        finish(n)

        @pl.when(n >= 2)
        def _():
            forward(n - 2)

    for n in range(max(tiles - 2, 0), tiles):
        forward(n)
    loads[6].wait()
    bytes_wait(hid.at[pl.ds(0, X)], rsem.at[9])

    DW = wd.shape[1]
    dsize = tile_of(DW, 256)

    parts = dsend.shape[0]
    span = DW // parts
    owns = []
    for p in range(parts):

        @pl.loop(0, span // dsize)
        def _(n):
            at = pl.multiple_of(n * dsize, 128)
            stage[:, pl.ds(at, dsize)] = jnp.dot(
                hid[...].reshape(N, FW),
                wd[:, pl.ds(pl.multiple_of(p * span + at, 128), dsize)],
                preferred_element_type=f32,
            )

        for g in range(G):
            dsend[p, g] = stage[g * R : (g + 1) * R, :span].astype(bf16)
        own = pltpu.make_async_copy(dsend.at[p, g_me], drecv.at[p, g_me], lsem.at[9 + p])
        own.start()
        owns.append(own)

        @pl.loop(1, G)
        def _(k):
            g = lax.rem(g_me + k, G)
            remote(
                dsend.at[p, g], drecv.at[p, g_me], 10, lax.div(g, T), lax.rem(g, T)
            ).start()

    for own in owns:
        own.wait()
    bytes_wait(drecv.at[:, pl.ds(0, G - 1)], rsem.at[10])
    for t in range(T):
        for p in range(parts):
            add = drecv[p, t].astype(f32)
            for c in range(1, C):
                add += drecv[p, c * T + t].astype(f32)
            cols = slice(t * DW + p * span, t * DW + (p + 1) * span)
            mixed_ref[:, cols] = (attended_ref[:, cols].astype(f32) + add).astype(bf16)

    bytes_wait(xrecv.at[pl.ds(0, G - 1)], ssem.at[0])
    bytes_wait(precv.at[pl.ds(0, C - 1)], ssem.at[1])
    bytes_wait(kvbuf.at[pl.ds(0, C - 1)], ssem.at[2])
    bytes_wait(abuf.at[pl.ds(0, C - 1)], ssem.at[3])
    bytes_wait(orecv.at[pl.ds(0, G - 1)], ssem.at[4])
    bytes_wait(nrecv.at[0, pl.ds(0, T - 1)], ssem.at[5])
    bytes_wait(nrecv.at[pl.ds(0, C - 1)], ssem.at[11])
    bytes_wait(g1recv, ssem.at[6])
    if X > 1:
        bytes_wait(g2recv, ssem.at[7])
        bytes_wait(hid.at[pl.ds(0, X - 1)], ssem.at[8])
    bytes_wait(hid.at[pl.ds(0, X)], ssem.at[9])
    bytes_wait(drecv.at[:, pl.ds(0, G - 1)], ssem.at[10])


def tables(count):
    half = HD // 2
    inverse = rope_base ** (-(np.arange(half, dtype=np.float64) * 2.0 / HD))
    angles = np.arange(count, dtype=np.float64)[:, None] * inverse[None, :]
    cos = np.concatenate([np.cos(angles), np.cos(angles)], axis=1)
    sin = np.concatenate([-np.sin(angles), np.sin(angles)], axis=1)
    return jnp.asarray(cos, f32), jnp.asarray(sin, f32)


def per_device(tokens, again, wq, wk, wv, wo, fgain, wg, wu, wd, *, T, C):
    R, D = tokens.shape
    G = T * C
    X = T // 2
    N = R * G
    B = R * T
    QW, KW, FW = wq.shape[1], wk.shape[1], wg.shape[1]
    DC, DT, OC, DW = wq.shape[0], wg.shape[0], wo.shape[1], wd.shape[1]
    cos, sin = tables(N)
    vm = pl.BlockSpec(memory_space=pltpu.VMEM)
    hbm = pl.BlockSpec(memory_space=pl.ANY)
    wide = max(DC, DT, OC, DW)
    tiles = FW // tile_of(FW)
    parts = 2 if DW % 512 == 0 else 1

    def buf(*shape, dtype=bf16):
        return pltpu.VMEM(shape, dtype)

    macs = N * sum(w.size for w in (wq, wk, wv, wo, wg, wu, wd))
    return pl.pallas_call(
        functools.partial(kernel, T, C),
        out_shape=(jax.ShapeDtypeStruct((R, D), bf16), jax.ShapeDtypeStruct((R, D), bf16)),
        in_specs=[vm] * 5 + [hbm] * 7,
        out_specs=(vm, vm),
        scratch_shapes=[
            *[buf(*w.shape) for w in (wq, wk, wv, wo, wg, wu, wd)],
            buf(C, R, DC),
            buf(G, R, DC),
            buf(N, max(DC, DT)),
            buf(N, wide, dtype=f32),
            buf(C, B, QW + 2 * KW),
            buf(C, B, QW + 2 * KW),
            buf(C, B, 2 * KW),
            buf(C, B, QW),
            buf(G, R, OC),
            buf(G, R, OC),
            buf(T, R, DT),
            buf(C, T, R, DT),
            buf(T, N // T, 2 * FW),
            buf(X, N // T, 2 * FW),
            buf(max(X - 1, 1), N // T, 2 * FW),
            buf(max(X - 1, 1), N // T, 2 * FW),
            buf(T, N // T, FW),
            buf(parts, G, R, DW // parts),
            buf(parts, G, R, DW // parts),
            pltpu.SemaphoreType.DMA((7,)),
            pltpu.SemaphoreType.DMA((12,)),
            pltpu.SemaphoreType.DMA((12,)),
            pltpu.SemaphoreType.DMA((12,)),
            pltpu.SemaphoreType.DMA((max(C // 2, 1),)),
            pltpu.SemaphoreType.DMA((max(C // 2, 1),)),
            pltpu.SemaphoreType.DMA((tiles,)),
            pltpu.SemaphoreType.DMA((tiles,)),
            pltpu.SemaphoreType.DMA((tiles,)),
        ],
        compiler_params=pltpu.CompilerParams(
            collective_id=0, has_side_effects=True, vmem_limit_bytes=67043328
        ),
        cost_estimate=pl.CostEstimate(flops=2 * macs, bytes_accessed=2 * macs // N, transcendentals=0),
    )(tokens, again.reshape(1, D), fgain.reshape(1, D), cos, sin, wq, wk, wv, wo, wg, wu, wd)


def solution(mesh):
    in_specs = (
        P(("cp", "tp"), None),
        P(),
        P("cp", "tp"),
        P("cp", "tp"),
        P("cp", "tp"),
        P("tp", "cp"),
        P(),
        P("tp", "cp"),
        P("tp", "cp"),
        P("cp", "tp"),
    )
    out_specs = (P(("cp", "tp"), None), P(("cp", "tp"), None))
    body = functools.partial(per_device, T=mesh.shape["tp"], C=mesh.shape["cp"])
    return jax.shard_map(body, mesh=mesh, in_specs=in_specs, out_specs=out_specs, check_vma=False)
```
